128 devices in a mesh: seq: 32 (over z, x, core), group: 4 (over y).
Axes of the slice: x: 4, y: 4, z: 4, core: 2. Of those that a mesh axis runs over, the one named last changes fastest.
Arguments:
- new_queries: bfloat16 [32, 8, 8, 128], P('seq', 'group'), may hold values from -6 to 6
- stored_keys: bfloat16 [32, 8, 16384, 128], P(None, 'group', 'seq'), may hold values from -6 to 6
- stored_values: bfloat16 [32, 8, 16384, 128], P(None, 'group', 'seq'), may hold values from -6 to 6
- used_length: int32 [32], replicated, may hold values from 8192 to 16384
- out_weight: bfloat16 [8, 8, 128, 5120], P('group'), may hold values from -0.0625 to 0.0625
Outputs:
- token_out: bfloat16 [32, 5120], P('seq', 'group')
The draws below stay inside these ranges and needn't reach their ends.
All inputs are finite; a program needn't handle non-finite values.
Results may differ from the reference program's by a relative error of at most 0.0025.
Values may be sent and summed in bfloat16 or wider, within the bound.
No kernel may reach another device: no remote copies, remote signals or barrier semaphores. Data moves between devices by JAX's collectives and lax.ppermute only.
A program may use at most 128 MiB of HBM per device.

```python
import jax
import jax.numpy as jnp
from jax import lax

BATCH = 32
LENGTH = 16384
KV_HEADS = 8
GROUP = 8
HEAD_SIZE = 128
D_MODEL = 5120


def plant(drawn, key, smallest, largest):
    place = [jax.random.randint(jax.random.fold_in(key, axis), (), 0, length) for axis, length in enumerate(drawn.shape)]
    longest = drawn.shape.index(max(drawn.shape))
    neighbour = place[:longest] + [(place[longest] + 1) % drawn.shape[longest]] + place[longest + 1:]
    return drawn.at[tuple(place)].set(smallest).at[tuple(neighbour)].set(largest)


def steps_of(rng, extent, shards, smallest, top_value):
    def one(axis_at, shards_of):
        draws = jax.random.uniform(jax.random.fold_in(jax.random.fold_in(rng, 6), axis_at), (shards_of,), jnp.float32, smallest / len(shards), top_value / len(shards))
        return jnp.repeat(jnp.exp(draws), extent[axis_at] // shards_of).reshape((-1,) + (1,) * (len(extent) - axis_at - 1))

    gain = one(*shards[0])
    for cut in shards[1:]:
        gain = gain * one(*cut)
    return gain


def scatter_about(own_key, shape, deviation, reach, split=(), kind=jnp.bfloat16):
    array = jax.random.normal(own_key, shape, jnp.float32) * deviation
    if len(split) > 0:
        array = steps_of(own_key, shape, split, -0.22, 0.18) * array
    return jnp.clip(array, min=-reach, max=reach).astype(kind)


def setup_inputs(seed: int = 0) -> dict:
    arg_keys = jax.random.split(jax.random.key(seed), 6)
    new_queries = scatter_about(arg_keys[0], (BATCH, KV_HEADS, GROUP, HEAD_SIZE), 1.0, 6.0, ((0, 32), (1, 4)))
    stored_keys = scatter_about(arg_keys[1], (BATCH, KV_HEADS, LENGTH, HEAD_SIZE), 1.0, 6.0, ((1, 4), (2, 32)))
    stored_values = scatter_about(arg_keys[2], (BATCH, KV_HEADS, LENGTH, HEAD_SIZE), 1.0, 6.0, ((1, 4), (2, 32)))
    used_length = plant(jax.random.randint(arg_keys[3], (BATCH,), LENGTH // 2, LENGTH + 1), jax.random.fold_in(arg_keys[3], 1), LENGTH // 2, LENGTH).astype(jnp.int32)
    out_weight = scatter_about(arg_keys[4], (KV_HEADS, GROUP, HEAD_SIZE, D_MODEL), (KV_HEADS * GROUP * HEAD_SIZE) ** -0.5, 0.0625, ((0, 4),))
    return {"new_queries": new_queries, "stored_keys": stored_keys, "stored_values": stored_values, "used_length": used_length, "out_weight": out_weight}


def reference(new_queries, stored_keys, stored_values, used_length, out_weight):
    def one_sequence(item):
        query_one, keys_one, values_one, length_one = item
        logit = jnp.einsum("kgd,ktd->kgt", query_one.astype(jnp.float32), keys_one.astype(jnp.float32)) * HEAD_SIZE ** -0.5
        logit = jnp.where(jnp.arange(LENGTH) < length_one, logit, -1e30)
        share = jax.nn.softmax(logit, axis=-1)
        return jnp.einsum("kgt,ktd->kgd", share, values_one.astype(jnp.float32), precision=lax.Precision.HIGHEST)
    read = lax.map(one_sequence, (new_queries, stored_keys, stored_values, used_length)).astype(jnp.bfloat16)
    read = lax.optimization_barrier(read)
    token_out = jnp.einsum("bkgd,kgdm->bm", read.astype(jnp.float32), out_weight.astype(jnp.float32)).astype(jnp.bfloat16)
    return token_out
```

```python
import jax
import jax.numpy as jnp
from jax import lax
from jax.sharding import PartitionSpec as P

HEAD_SIZE = 128


def per_device(new_queries, stored_keys, stored_values, used_length, out_weight):
    batch = stored_keys.shape[0]
    copies = jnp.broadcast_to(new_queries, (batch,) + new_queries.shape[1:])
    all_queries = lax.all_to_all(copies, "seq", split_axis=0, concat_axis=0, tiled=True)
    logit = jnp.einsum(
        "bkgd,bktd->bkgt", all_queries, stored_keys, preferred_element_type=jnp.float32
    ) * HEAD_SIZE ** (-0.5)
    positions = lax.axis_index("seq") * stored_keys.shape[2] + jnp.arange(stored_keys.shape[2])
    filled = positions[None, :] < used_length[:, None]
    logit = jnp.where(filled[:, None, None, :], logit, -1e30)
    top = jnp.max(logit, axis=-1)
    part = jnp.where(filled[:, None, None, :], jnp.exp(logit - top[..., None]), 0.0)
    weight_sum = jnp.sum(part, axis=-1)
    read_sum = jnp.einsum(
        "bkgt,bktd->bkgd", part, stored_values.astype(jnp.float32), precision=lax.Precision.HIGHEST
    )
    rows = read_sum.shape[1] * read_sum.shape[2]
    stats = jnp.stack([top.reshape(batch, rows), weight_sum.reshape(batch, rows)], axis=1)
    stats = jnp.pad(stats, ((0, 0), (0, 6), (0, HEAD_SIZE - rows)))
    packed = jnp.concatenate([read_sum.reshape(batch, rows, HEAD_SIZE), stats], axis=1)
    arrived = lax.all_to_all(packed, "seq", split_axis=0, concat_axis=0, tiled=True)
    tops, sums = arrived[:, rows, :rows], arrived[:, rows + 1, :rows]
    best = jnp.max(tops, axis=0)
    scale = jnp.exp(tops - best)
    weight_own = jnp.sum(sums * scale, axis=0)
    read_own = jnp.sum(arrived[:, :rows] * scale[..., None], axis=0)
    read = (read_own / weight_own[..., None]).astype(jnp.bfloat16)
    width = out_weight.shape[-1]
    term = jnp.dot(
        read.reshape(1, rows * HEAD_SIZE),
        out_weight.reshape(rows * HEAD_SIZE, width),
        preferred_element_type=jnp.float32,
    )
    shares = lax.axis_size("group")
    pieces = lax.all_to_all(
        term.reshape(shares, width // shares), "group", split_axis=0, concat_axis=0, tiled=True
    )
    return jnp.sum(pieces, axis=0, keepdims=True).astype(jnp.bfloat16)


def solution(mesh):
    in_specs = (
        P("seq", "group", None, None),
        P(None, "group", "seq", None),
        P(None, "group", "seq", None),
        P(),
        P("group", None, None, None),
    )
    out_specs = P("seq", "group")
    return jax.shard_map(
        per_device, mesh=mesh, in_specs=in_specs, out_specs=out_specs, check_vma=False
    )
```

```python
import functools

import jax
import jax.numpy as jnp
from jax import lax
from jax.experimental import pallas as pl
from jax.experimental.pallas import tpu as pltpu
from jax.sharding import PartitionSpec as P

HEAD_SIZE = 128
EMPTY = -1e30
TO_BASE_2 = HEAD_SIZE ** (-0.5) * 1.4426950408889634


def attend(used_ref, query_ref, key_ref, value_ref, out_ref):
    batch, heads, width, _ = key_ref.shape
    group = query_ref.shape[2]
    rows = heads * group
    first = lax.axis_index("seq") * width
    lane = lax.broadcasted_iota(jnp.int32, (group, HEAD_SIZE), 1)
    sub = lax.broadcasted_iota(jnp.int32, (group, HEAD_SIZE), 0)
    place = lax.broadcasted_iota(jnp.int32, (group, width), 1)

    def one(b, carry):
        filled = place < used_ref[b] - first
        stats = jnp.zeros((group, HEAD_SIZE), jnp.float32)
        for k in range(heads):
            logit = lax.dot_general(
                query_ref[b, k], key_ref[b, k], (((1,), (1,)), ((), ())),
                preferred_element_type=jnp.float32,
            )
            logit = jnp.where(filled, logit * TO_BASE_2, EMPTY)
            top = jnp.max(logit, axis=1, keepdims=True)
            part = jnp.where(filled, jnp.exp2(logit - top), 0.0)
            total = jnp.sum(part, axis=1, keepdims=True)
            high = part.astype(jnp.bfloat16)
            low = (part - high.astype(jnp.float32)).astype(jnp.bfloat16)
            both = jnp.dot(
                jnp.concatenate([high, low], axis=0), value_ref[b, k],
                preferred_element_type=jnp.float32,
            )
            out_ref[b, pl.ds(k * group, group), :] = both[:group] + both[group:]
            stats = jnp.where(lane == sub + k * group, top, stats)
            stats = jnp.where(lane == sub + (rows + k * group), total, stats)
        out_ref[b, pl.ds(rows, 8), :] = jnp.broadcast_to(
            jnp.sum(stats, axis=0, keepdims=True), (8, HEAD_SIZE)
        )
        return carry

    lax.fori_loop(0, batch, one, 0, unroll=4)


def project(arrived_ref, weight_ref, out_ref):
    sources = arrived_ref.shape[0]
    rows = weight_ref.shape[0] // HEAD_SIZE
    stats = jnp.transpose(arrived_ref[:, rows, :])
    tops, sums = stats[:rows], stats[rows : 2 * rows]
    scale = jnp.exp2(tops - jnp.max(tops, axis=1, keepdims=True))
    scale = scale / jnp.sum(sums * scale, axis=1, keepdims=True)
    read = jnp.zeros((rows, HEAD_SIZE), jnp.float32)
    for s in range(sources):
        read = read + arrived_ref[s, pl.ds(0, rows), :] * scale[:, s : s + 1]
    row = lax.broadcasted_iota(jnp.int32, (rows, HEAD_SIZE), 0)
    left = jnp.concatenate(
        [jnp.where(row == r, read, 0.0).astype(jnp.bfloat16) for r in range(rows)], axis=1
    )
    step = 512

    def columns(n, carry):
        at = pl.ds(pl.multiple_of(n * step, step), step)
        term = jnp.dot(left, weight_ref[:, at], preferred_element_type=jnp.float32)
        out_ref[:, at] = jnp.sum(term, axis=0, keepdims=True)
        return carry

    lax.fori_loop(0, weight_ref.shape[1] // step, columns, 0)


def per_device(new_queries, stored_keys, stored_values, used_length, out_weight):
    batch, heads = stored_keys.shape[:2]
    group = new_queries.shape[2]
    rows = heads * group
    width = out_weight.shape[-1]
    vmem = functools.partial(pltpu.with_memory_space_constraint, memory_space=pltpu.VMEM)
    whole = pl.BlockSpec(memory_space=pltpu.VMEM)

    copies = jnp.broadcast_to(new_queries, (batch,) + new_queries.shape[1:])
    all_queries = lax.all_to_all(copies, "seq", split_axis=0, concat_axis=0, tiled=True)
    packed = pl.pallas_call(
        attend,
        out_shape=jax.ShapeDtypeStruct((batch, rows + 8, HEAD_SIZE), jnp.float32),
        in_specs=[pl.BlockSpec(memory_space=pltpu.SMEM), whole, whole, whole],
        out_specs=whole,
        compiler_params=pltpu.CompilerParams(vmem_limit_bytes=8 << 20),
        name="attend",
    )(used_length, vmem(all_queries), vmem(stored_keys), vmem(stored_values))
    arrived = lax.all_to_all(packed, "seq", split_axis=0, concat_axis=0, tiled=True)
    term = pl.pallas_call(
        project,
        out_shape=jax.ShapeDtypeStruct((1, width), jnp.float32),
        in_specs=[whole, whole],
        out_specs=whole,
        compiler_params=pltpu.CompilerParams(vmem_limit_bytes=8 << 20),
        name="project",
    )(vmem(arrived), vmem(out_weight.reshape(rows * HEAD_SIZE, width)))
    shares = lax.axis_size("group")
    pieces = lax.all_to_all(
        term.reshape(shares, 1, width // shares), "group", split_axis=0, concat_axis=0, tiled=True
    )
    return jnp.sum(pieces, axis=0).astype(jnp.bfloat16)


def solution(mesh):
    in_specs = (
        P("seq", "group", None, None),
        P(None, "group", "seq", None),
        P(None, "group", "seq", None),
        P(),
        P("group", None, None, None),
    )
    out_specs = P("seq", "group")
    return jax.shard_map(
        per_device, mesh=mesh, in_specs=in_specs, out_specs=out_specs, check_vma=False
    )
```

```python
import functools

import jax
import jax.numpy as jnp
from jax import lax
from jax.experimental import pallas as pl
from jax.experimental.pallas import tpu as pltpu
from jax.sharding import PartitionSpec as P

HEAD_SIZE = 128
EMPTY = -1e30
BLOCK = 8
TO_BASE_2 = HEAD_SIZE ** (-0.5) * 1.4426950408889634


def attend(used_ref, query_ref, key_ref, value_ref, out_ref):
    batch, heads, width, _ = key_ref.shape
    rows = query_ref.shape[1]
    group = rows // heads
    first = lax.axis_index("seq") * width
    lane = lax.broadcasted_iota(jnp.int32, (rows, HEAD_SIZE), 1)
    row = lax.broadcasted_iota(jnp.int32, (rows, HEAD_SIZE), 0)
    place = lax.broadcasted_iota(jnp.int32, (rows, width), 1)

    def side_by_side(ref, b):
        return jnp.concatenate([ref[b, k] for k in range(heads)], axis=1)

    def block(i, carry):
        at = [i * BLOCK + j for j in range(BLOCK)]
        logits = []
        for b in at:
            query = query_ref[b].astype(jnp.float32)
            left = jnp.concatenate(
                [jnp.where(row // group == k, query, 0.0) for k in range(heads)], axis=1
            ).astype(jnp.bfloat16)
            logits.append(
                lax.dot_general(
                    left, side_by_side(key_ref, b), (((1,), (1,)), ((), ())),
                    preferred_element_type=jnp.float32,
                )
            )
        filled = [place < used_ref[b] - first for b in at]
        logits = [jnp.where(f, x * TO_BASE_2, EMPTY) for f, x in zip(filled, logits)]
        tops = [jnp.max(x, axis=1, keepdims=True) for x in logits]
        parts = [jnp.where(f, jnp.exp2(x - t), 0.0) for f, x, t in zip(filled, logits, tops)]
        totals = [jnp.sum(p, axis=1, keepdims=True) for p in parts]
        reads = []
        for b, part in zip(at, parts):
            high = part.astype(jnp.bfloat16)
            low = (part - high.astype(jnp.float32)).astype(jnp.bfloat16)
            both = jnp.dot(
                jnp.concatenate([high, low], axis=0), side_by_side(value_ref, b),
                preferred_element_type=jnp.float32,
            )
            reads.append(both[:rows] + both[rows:])
        for b, read, top, total in zip(at, reads, tops, totals):
            for k in range(heads):
                out_ref[b, pl.ds(k * group, group), :] = read[
                    k * group : (k + 1) * group, k * HEAD_SIZE : (k + 1) * HEAD_SIZE
                ]
            stats = jnp.where(lane == row, top, jnp.where(lane == row + rows, total, 0.0))
            out_ref[b, pl.ds(rows, 8), :] = jnp.broadcast_to(
                jnp.sum(stats, axis=0, keepdims=True), (8, HEAD_SIZE)
            )
        return carry

    lax.fori_loop(0, batch // BLOCK, block, 0)


def spread(one_ref, out_ref):
    out_ref[...] = jnp.broadcast_to(one_ref[...], out_ref.shape)


def project(arrived_ref, weight_ref, out_ref):
    sources = arrived_ref.shape[0]
    rows = weight_ref.shape[0] // HEAD_SIZE
    stats = jnp.transpose(arrived_ref[:, rows, :])
    tops, sums = stats[:rows], stats[rows : 2 * rows]
    scale = jnp.exp2(tops - jnp.max(tops, axis=1, keepdims=True))
    scale = scale / jnp.sum(sums * scale, axis=1, keepdims=True)
    read = jnp.zeros((rows, HEAD_SIZE), jnp.float32)
    for s in range(sources):
        read = read + arrived_ref[s, pl.ds(0, rows), :] * scale[:, s : s + 1]
    row = lax.broadcasted_iota(jnp.int32, (rows, HEAD_SIZE), 0)
    left = jnp.concatenate(
        [jnp.where(row == r, read, 0.0).astype(jnp.bfloat16) for r in range(rows)], axis=1
    )
    step = 512

    def columns(n, carry):
        at = pl.ds(pl.multiple_of(n * step, step), step)
        term = jnp.dot(left, weight_ref[:, at], preferred_element_type=jnp.float32)
        out_ref[:, at] = jnp.sum(term, axis=0, keepdims=True)
        return carry

    lax.fori_loop(0, weight_ref.shape[1] // step, columns, 0)


def per_device(new_queries, stored_keys, stored_values, used_length, out_weight):
    batch, heads = stored_keys.shape[:2]
    group = new_queries.shape[2]
    rows = heads * group
    width = out_weight.shape[-1]
    vmem = functools.partial(pltpu.with_memory_space_constraint, memory_space=pltpu.VMEM)
    whole = pl.BlockSpec(memory_space=pltpu.VMEM)

    queries = new_queries.reshape(1, rows, HEAD_SIZE)
    copies = pl.pallas_call(
        spread,
        out_shape=jax.ShapeDtypeStruct((batch, rows, HEAD_SIZE), queries.dtype),
        in_specs=[whole],
        out_specs=whole,
        cost_estimate=pl.CostEstimate(flops=10**11, bytes_accessed=10**9, transcendentals=0),
        compiler_params=pltpu.CompilerParams(vmem_limit_bytes=1 << 20),
        name="spread",
    )(queries)
    all_queries = lax.all_to_all(copies, "seq", split_axis=0, concat_axis=0, tiled=True)
    packed = pl.pallas_call(
        attend,
        out_shape=jax.ShapeDtypeStruct((batch, rows + 8, HEAD_SIZE), jnp.float32),
        in_specs=[pl.BlockSpec(memory_space=pltpu.SMEM), whole, whole, whole],
        out_specs=whole,
        compiler_params=pltpu.CompilerParams(vmem_limit_bytes=8 << 20),
        name="attend",
    )(used_length, vmem(all_queries), vmem(stored_keys), vmem(stored_values))
    arrived = lax.all_to_all(packed, "seq", split_axis=0, concat_axis=0, tiled=True)
    term = pl.pallas_call(
        project,
        out_shape=jax.ShapeDtypeStruct((1, width), jnp.float32),
        in_specs=[whole, whole],
        out_specs=whole,
        compiler_params=pltpu.CompilerParams(vmem_limit_bytes=8 << 20),
        name="project",
    )(vmem(arrived), vmem(out_weight.reshape(rows * HEAD_SIZE, width)))
    shares = lax.axis_size("group")
    pieces = lax.all_to_all(
        term.reshape(shares, 1, width // shares), "group", split_axis=0, concat_axis=0, tiled=True
    )
    return jnp.sum(pieces, axis=0).astype(jnp.bfloat16)


def solution(mesh):
    in_specs = (
        P("seq", "group", None, None),
        P(None, "group", "seq", None),
        P(None, "group", "seq", None),
        P(),
        P("group", None, None, None),
    )
    out_specs = P("seq", "group")
    return jax.shard_map(
        per_device, mesh=mesh, in_specs=in_specs, out_specs=out_specs, check_vma=False
    )
```

```python
import functools

import jax
import jax.numpy as jnp
from jax import lax
from jax.experimental import pallas as pl
from jax.experimental.pallas import tpu as pltpu
from jax.sharding import PartitionSpec as P

HEAD_SIZE = 128
EMPTY = -1e30
BLOCK = 8
STEP = 256
ORDER = (2, 3, 1, 0)
TO_BASE_2 = HEAD_SIZE ** (-0.5) * 1.4426950408889634


def attend(used_ref, query_ref, key_ref, value_ref, out_ref):
    batch, heads, width, _ = key_ref.shape
    rows = query_ref.shape[1]
    group = rows // heads
    first = lax.axis_index("seq") * width
    lane = lax.broadcasted_iota(jnp.int32, (rows, HEAD_SIZE), 1)
    row = lax.broadcasted_iota(jnp.int32, (rows, HEAD_SIZE), 0)
    place = lax.broadcasted_iota(jnp.int32, (rows, width), 1)

    def side_by_side(ref, b):
        return jnp.concatenate([ref[b, k] for k in range(heads)], axis=1)

    def block(i, carry):
        at = [i * BLOCK + j for j in range(BLOCK)]
        logits = []
        for b in at:
            query = query_ref[b].astype(jnp.float32)
            left = jnp.concatenate(
                [jnp.where(row // group == k, query, 0.0) for k in range(heads)], axis=1
            ).astype(jnp.bfloat16)
            logits.append(
                lax.dot_general(
                    left, side_by_side(key_ref, b), (((1,), (1,)), ((), ())),
                    preferred_element_type=jnp.float32,
                )
            )
        filled = [place < used_ref[b] - first for b in at]
        logits = [jnp.where(f, x * TO_BASE_2, EMPTY) for f, x in zip(filled, logits)]
        tops = [jnp.max(x, axis=1, keepdims=True) for x in logits]
        parts = [jnp.where(f, jnp.exp2(x - t), 0.0) for f, x, t in zip(filled, logits, tops)]
        totals = [jnp.sum(p, axis=1, keepdims=True) for p in parts]
        reads = []
        for b, part in zip(at, parts):
            high = part.astype(jnp.bfloat16)
            low = (part - high.astype(jnp.float32)).astype(jnp.bfloat16)
            both = jnp.dot(
                jnp.concatenate([high, low], axis=0), side_by_side(value_ref, b),
                preferred_element_type=jnp.float32,
            )
            reads.append(both[:rows] + both[rows:])
        for b, read, top, total in zip(at, reads, tops, totals):
            for k in range(heads):
                out_ref[pl.ds(b * (rows + 1) + k * group, group), :] = read[
                    k * group : (k + 1) * group, k * HEAD_SIZE : (k + 1) * HEAD_SIZE
                ]
            stats = jnp.where(lane == row, top, jnp.where(lane == row + rows, total, 0.0))
            out_ref[pl.ds(b * (rows + 1) + rows, 1), :] = jnp.sum(stats, axis=0, keepdims=True)
        return carry

    lax.fori_loop(0, batch // BLOCK, block, 0)


def spread(one_ref, out_ref):
    out_ref[...] = jnp.broadcast_to(one_ref[...], out_ref.shape)


def merge(arrived_ref, rows):
    sources = arrived_ref.shape[0] // (rows + 1)
    stats = jnp.transpose(arrived_ref[pl.ds(rows, sources, stride=rows + 1), :])
    tops, sums = stats[:rows], stats[rows : 2 * rows]
    scale = jnp.exp2(tops - jnp.max(tops, axis=1, keepdims=True))
    scale = scale / jnp.sum(sums * scale, axis=1, keepdims=True)
    read = jnp.zeros((rows, HEAD_SIZE), jnp.float32)
    for s in range(sources):
        read = read + arrived_ref[pl.ds(s * (rows + 1), rows), :] * scale[:, s : s + 1]
    row = lax.broadcasted_iota(jnp.int32, (rows, HEAD_SIZE), 0)
    return jnp.concatenate(
        [jnp.where(row == r, read, 0.0).astype(jnp.bfloat16) for r in range(rows)], axis=1
    )


def columns(left, weight_ref, share, out_ref):
    width = out_ref.shape[-1]
    for n in range(0, width, STEP):
        at = pl.ds(pl.multiple_of(share * width + n, STEP), STEP)
        term = jnp.dot(left, weight_ref[:, at], preferred_element_type=jnp.float32)
        out_ref[:, pl.ds(n, STEP)] = jnp.sum(term, axis=0, keepdims=True)


def project_first(away, arrived_ref, weight_ref, left_ref, out_ref):
    left = merge(arrived_ref, weight_ref.shape[0] // HEAD_SIZE)
    left_ref[...] = left
    columns(left, weight_ref, lax.axis_index("group") ^ away, out_ref)


def project_next(away, left_ref, weight_ref, out_ref):
    columns(left_ref[...], weight_ref, lax.axis_index("group") ^ away, out_ref)


def add_all(own_ref, a_ref, b_ref, c_ref, out_ref):
    total = (own_ref[...] + a_ref[...]) + (b_ref[...] + c_ref[...])
    out_ref[...] = total.astype(out_ref.dtype)


def per_device(new_queries, stored_keys, stored_values, used_length, out_weight):
    batch, heads = stored_keys.shape[:2]
    group = new_queries.shape[2]
    rows = heads * group
    width = out_weight.shape[-1]
    vmem = functools.partial(pltpu.with_memory_space_constraint, memory_space=pltpu.VMEM)
    whole = pl.BlockSpec(memory_space=pltpu.VMEM)

    queries = new_queries.reshape(1, rows, HEAD_SIZE)
    copies = pl.pallas_call(
        spread,
        out_shape=jax.ShapeDtypeStruct((batch, rows, HEAD_SIZE), queries.dtype),
        in_specs=[whole],
        out_specs=whole,
        cost_estimate=pl.CostEstimate(flops=10**11, bytes_accessed=10**9, transcendentals=0),
        compiler_params=pltpu.CompilerParams(vmem_limit_bytes=1 << 20),
        name="spread",
    )(queries)
    all_queries = lax.all_to_all(copies, "seq", split_axis=0, concat_axis=0, tiled=True)
    packed = pl.pallas_call(
        attend,
        out_shape=jax.ShapeDtypeStruct((batch * (rows + 1), HEAD_SIZE), jnp.float32),
        in_specs=[pl.BlockSpec(memory_space=pltpu.SMEM), whole, whole, whole],
        out_specs=whole,
        compiler_params=pltpu.CompilerParams(vmem_limit_bytes=8 << 20),
        name="attend",
    )(used_length, vmem(all_queries), vmem(stored_keys), vmem(stored_values))
    arrived = lax.all_to_all(
        packed.reshape(batch, rows + 1, 1, HEAD_SIZE), "seq", split_axis=0, concat_axis=0, tiled=True
    ).reshape(packed.shape)
    shares = lax.axis_size("group")
    piece = jax.ShapeDtypeStruct((1, width // shares), jnp.float32)
    small = pltpu.CompilerParams(vmem_limit_bytes=8 << 20)
    cost = pl.CostEstimate(flops=10**9, bytes_accessed=10**7, transcendentals=0)
    weight = vmem(out_weight.reshape(rows * HEAD_SIZE, width))
    left, term = pl.pallas_call(
        functools.partial(project_first, ORDER[0]),
        out_shape=(jax.ShapeDtypeStruct((rows, rows * HEAD_SIZE), jnp.bfloat16), piece),
        in_specs=[whole, whole],
        out_specs=(whole, whole),
        compiler_params=small,
        name="project_first",
    )(vmem(arrived), weight)
    pieces = []
    for n, away in enumerate(ORDER[1:]):
        pieces.append(
            lax.ppermute(term, "group", [(j, j ^ ORDER[n]) for j in range(shares)])
        )
        term = pl.pallas_call(
            functools.partial(project_next, away),
            out_shape=piece,
            in_specs=[whole, whole],
            out_specs=whole,
            cost_estimate=cost,
            compiler_params=small,
            name="project_next",
        )(left, weight)
    return pl.pallas_call(
        add_all,
        out_shape=jax.ShapeDtypeStruct(piece.shape, jnp.bfloat16),
        in_specs=[whole] * 4,
        out_specs=whole,
        compiler_params=small,
        name="add_all",
    )(term, *pieces)


def solution(mesh):
    in_specs = (
        P("seq", "group", None, None),
        P(None, "group", "seq", None),
        P(None, "group", "seq", None),
        P(),
        P("group", None, None, None),
    )
    out_specs = P("seq", "group")
    return jax.shard_map(
        per_device, mesh=mesh, in_specs=in_specs, out_specs=out_specs, check_vma=False
    )
```

```python
import functools

import jax
import jax.numpy as jnp
from jax import lax
from jax.experimental import pallas as pl
from jax.experimental.pallas import tpu as pltpu
from jax.sharding import PartitionSpec as P

HEAD_SIZE = 128
EMPTY = -1e30
BLOCK = 32
STEP = 256
NEAR, LAST = 1, 3
TO_BASE_2 = HEAD_SIZE ** (-0.5) * 1.4426950408889634


def attend(used_ref, query_ref, key_ref, value_ref, out_ref):
    batch, heads, width, _ = key_ref.shape
    rows = query_ref.shape[1]
    group = rows // heads
    first = lax.axis_index("seq") * width
    lane = lax.broadcasted_iota(jnp.int32, (rows, HEAD_SIZE), 1)
    row = lax.broadcasted_iota(jnp.int32, (rows, HEAD_SIZE), 0)
    place = lax.broadcasted_iota(jnp.int32, (rows, width), 1)

    def side_by_side(ref, b):
        return jnp.concatenate([ref[b, k] for k in range(heads)], axis=1)

    def block(i, carry):
        at = [i * BLOCK + j for j in range(BLOCK)]
        logits = []
        for b in at:
            query = query_ref[b].astype(jnp.float32)
            left = jnp.concatenate(
                [jnp.where(row // group == k, query, 0.0) for k in range(heads)], axis=1
            ).astype(jnp.bfloat16)
            logits.append(
                lax.dot_general(
                    left, side_by_side(key_ref, b), (((1,), (1,)), ((), ())),
                    preferred_element_type=jnp.float32,
                )
            )
        filled = [place < used_ref[b] - first for b in at]
        logits = [jnp.where(f, x * TO_BASE_2, EMPTY) for f, x in zip(filled, logits)]
        tops = [jnp.max(x, axis=1, keepdims=True) for x in logits]
        parts = [jnp.where(f, jnp.exp2(x - t), 0.0) for f, x, t in zip(filled, logits, tops)]
        totals = [jnp.sum(p, axis=1, keepdims=True) for p in parts]
        reads = []
        for b, part in zip(at, parts):
            high = part.astype(jnp.bfloat16)
            low = (part - high.astype(jnp.float32)).astype(jnp.bfloat16)
            both = jnp.dot(
                jnp.concatenate([high, low], axis=0), side_by_side(value_ref, b),
                preferred_element_type=jnp.float32,
            )
            reads.append(both[:rows] + both[rows:])
        for b, read, top, total in zip(at, reads, tops, totals):
            for k in range(heads):
                out_ref[pl.ds(b * (rows + 1) + k * group, group), :] = read[
                    k * group : (k + 1) * group, k * HEAD_SIZE : (k + 1) * HEAD_SIZE
                ]
            stats = jnp.where(lane == row, top, jnp.where(lane == row + rows, total, 0.0))
            out_ref[pl.ds(b * (rows + 1) + rows, 1), :] = jnp.sum(stats, axis=0, keepdims=True)
        return carry

    lax.fori_loop(0, batch // BLOCK, block, 0)


def spread(one_ref, out_ref):
    out_ref[...] = jnp.broadcast_to(one_ref[...], out_ref.shape)


def merge(arrived_ref, rows):
    sources = arrived_ref.shape[0] // (rows + 1)
    stats = jnp.transpose(arrived_ref[pl.ds(rows, sources, stride=rows + 1), :])
    tops, sums = stats[:rows], stats[rows : 2 * rows]
    scale = jnp.exp2(tops - jnp.max(tops, axis=1, keepdims=True))
    scale = scale / jnp.sum(sums * scale, axis=1, keepdims=True)
    read = jnp.zeros((rows, HEAD_SIZE), jnp.float32)
    for s in range(sources):
        read = read + arrived_ref[pl.ds(s * (rows + 1), rows), :] * scale[:, s : s + 1]
    row = lax.broadcasted_iota(jnp.int32, (rows, HEAD_SIZE), 0)
    return jnp.concatenate(
        [jnp.where(row == r, read, 0.0).astype(jnp.bfloat16) for r in range(rows)], axis=1
    )


def columns(left, weight_ref, share, out_ref):
    width = out_ref.shape[-1]
    for n in range(0, width, STEP):
        at = pl.ds(pl.multiple_of(share * width + n, STEP), STEP)
        term = jnp.dot(left, weight_ref[:, at], preferred_element_type=jnp.float32)
        out_ref[:, pl.ds(n, STEP)] = jnp.sum(term, axis=0, keepdims=True)


def project_first(away, arrived_ref, weight_ref, left_ref, out_ref):
    left = merge(arrived_ref, weight_ref.shape[0] // HEAD_SIZE)
    left_ref[...] = left
    columns(left, weight_ref, lax.axis_index("group") ^ away, out_ref)


def project_next(away, left_ref, weight_ref, out_ref):
    columns(left_ref[...], weight_ref, lax.axis_index("group") ^ away, out_ref)


def add_all(*refs):
    out_ref = refs[-1]
    total = refs[0][...]
    for ref in refs[1:-1]:
        total = total + ref[...]
    out_ref[...] = total.astype(out_ref.dtype)


def per_device(new_queries, stored_keys, stored_values, used_length, out_weight):
    batch, heads = stored_keys.shape[:2]
    group = new_queries.shape[2]
    rows = heads * group
    width = out_weight.shape[-1]
    vmem = functools.partial(pltpu.with_memory_space_constraint, memory_space=pltpu.VMEM)
    whole = pl.BlockSpec(memory_space=pltpu.VMEM)

    queries = new_queries.reshape(1, rows, HEAD_SIZE)
    copies = pl.pallas_call(
        spread,
        out_shape=jax.ShapeDtypeStruct((batch, rows, HEAD_SIZE), queries.dtype),
        in_specs=[whole],
        out_specs=whole,
        cost_estimate=pl.CostEstimate(flops=10**11, bytes_accessed=10**9, transcendentals=0),
        compiler_params=pltpu.CompilerParams(vmem_limit_bytes=1 << 20),
        name="spread",
    )(queries)
    all_queries = lax.all_to_all(copies, "seq", split_axis=0, concat_axis=0, tiled=True)
    packed = pl.pallas_call(
        attend,
        out_shape=jax.ShapeDtypeStruct((batch * (rows + 1), HEAD_SIZE), jnp.float32),
        in_specs=[pl.BlockSpec(memory_space=pltpu.SMEM), whole, whole, whole],
        out_specs=whole,
        compiler_params=pltpu.CompilerParams(vmem_limit_bytes=8 << 20),
        name="attend",
    )(used_length, vmem(all_queries), vmem(stored_keys), vmem(stored_values))
    arrived = lax.all_to_all(
        packed.reshape(batch, rows + 1, 1, HEAD_SIZE), "seq", split_axis=0, concat_axis=0, tiled=True
    ).reshape(packed.shape)
    shares = lax.axis_size("group")
    piece = jax.ShapeDtypeStruct((1, width // shares), jnp.float32)
    small = pltpu.CompilerParams(vmem_limit_bytes=8 << 20)
    cost = pl.CostEstimate(flops=10**9, bytes_accessed=10**7, transcendentals=0)
    weight = vmem(out_weight.reshape(rows * HEAD_SIZE, width))
    left, term = pl.pallas_call(
        functools.partial(project_first, NEAR ^ LAST),
        out_shape=(jax.ShapeDtypeStruct((rows, rows * HEAD_SIZE), jnp.bfloat16), piece),
        in_specs=[whole, whole],
        out_specs=(whole, whole),
        compiler_params=small,
        name="project_first",
    )(vmem(arrived), weight)

    def send(term, away):
        return lax.ppermute(term, "group", [(j, j ^ away) for j in range(shares)])

    def following(away):
        return pl.pallas_call(
            functools.partial(project_next, away),
            out_shape=piece,
            in_specs=[whole, whole],
            out_specs=whole,
            cost_estimate=cost,
            compiler_params=small,
            name="project_next",
        )(left, weight)

    def added(parts, dtype):
        return pl.pallas_call(
            add_all,
            out_shape=jax.ShapeDtypeStruct(piece.shape, dtype),
            in_specs=[whole] * len(parts),
            out_specs=whole,
            compiler_params=small,
        )(*parts)

    passed = send(term, NEAR)
    direct = send(following(NEAR), NEAR)
    beyond = following(LAST)
    last = send(added([beyond, passed], jnp.float32), LAST)
    own = following(0)
    return added([own, direct, last], jnp.bfloat16)


def solution(mesh):
    in_specs = (
        P("seq", "group", None, None),
        P(None, "group", "seq", None),
        P(None, "group", "seq", None),
        P(),
        P("group", None, None, None),
    )
    out_specs = P("seq", "group")
    return jax.shard_map(
        per_device, mesh=mesh, in_specs=in_specs, out_specs=out_specs, check_vma=False
    )
```

```python
import functools

import jax
import jax.numpy as jnp
from jax import lax
from jax.experimental import pallas as pl
from jax.experimental.pallas import tpu as pltpu
from jax.sharding import PartitionSpec as P

HEAD_SIZE = 128
EMPTY = -1e30
STEP = 256
NEAR, LAST = 1, 3
TO_BASE_2 = HEAD_SIZE ** (-0.5) * 1.4426950408889634


def attend(used_ref, query_ref, key_ref, value_ref, out_ref):
    batch, heads, width, _ = key_ref.shape
    rows = query_ref.shape[1]
    group = rows // heads
    first = lax.axis_index("seq") * width
    lane = lax.broadcasted_iota(jnp.int32, (rows, HEAD_SIZE), 1)
    row = lax.broadcasted_iota(jnp.int32, (rows, HEAD_SIZE), 0)
    place = lax.broadcasted_iota(jnp.int32, (rows, width), 1)

    def side_by_side(ref, b):
        return jnp.concatenate([ref[b, k] for k in range(heads)], axis=1)

    used = used_ref[...] - first
    at = range(batch)
    logits = []
    for b in at:
        query = query_ref[b].astype(jnp.float32)
        left = jnp.concatenate(
            [jnp.where(row // group == k, query, 0.0) for k in range(heads)], axis=1
        ).astype(jnp.bfloat16)
        logits.append(
            lax.dot_general(
                left, side_by_side(key_ref, b), (((1,), (1,)), ((), ())),
                preferred_element_type=jnp.float32,
            )
        )
    filled = [place < used[:, b : b + 1] for b in at]
    logits = [jnp.where(f, x * TO_BASE_2, EMPTY) for f, x in zip(filled, logits)]
    tops = [jnp.max(x, axis=1, keepdims=True) for x in logits]
    parts = [jnp.where(f, jnp.exp2(x - t), 0.0) for f, x, t in zip(filled, logits, tops)]
    totals = [jnp.sum(p, axis=1, keepdims=True) for p in parts]
    reads = []
    for b, part in zip(at, parts):
        high = part.astype(jnp.bfloat16)
        low = (part - high.astype(jnp.float32)).astype(jnp.bfloat16)
        both = jnp.dot(
            jnp.concatenate([high, low], axis=0), side_by_side(value_ref, b),
            preferred_element_type=jnp.float32,
        )
        reads.append(both[:rows] + both[rows:])
    for b, read, top, total in zip(at, reads, tops, totals):
        for k in range(heads):
            out_ref[pl.ds(b * (rows + 1) + k * group, group), :] = read[
                k * group : (k + 1) * group, k * HEAD_SIZE : (k + 1) * HEAD_SIZE
            ]
        stats = jnp.where(lane == row, top, jnp.where(lane == row + rows, total, 0.0))
        out_ref[pl.ds(b * (rows + 1) + rows, 1), :] = jnp.sum(stats, axis=0, keepdims=True)


def spread(one_ref, out_ref):
    out_ref[...] = jnp.broadcast_to(one_ref[...], out_ref.shape)


def merge(arrived_ref, rows):
    sources = arrived_ref.shape[0] // (rows + 1)
    tops = arrived_ref[pl.ds(rows, sources, stride=rows + 1), :]
    sums = pltpu.roll(tops, HEAD_SIZE - rows, 1)
    scale = jnp.exp2(tops - jnp.max(tops, axis=0, keepdims=True))
    total = jnp.sum(sums * scale, axis=0, keepdims=True)
    lane = lax.broadcasted_iota(jnp.int32, total.shape, 1)
    scale = scale / jnp.where(lane < rows, total, 1.0)
    scale = jnp.transpose(scale)[:rows]
    terms = [
        arrived_ref[pl.ds(s * (rows + 1), rows), :] * scale[:, s : s + 1] for s in range(sources)
    ]
    while len(terms) > 1:
        terms = [a + b for a, b in zip(terms[::2], terms[1::2])]
    read = terms[0]
    row = lax.broadcasted_iota(jnp.int32, (rows, HEAD_SIZE), 0)
    return jnp.concatenate(
        [jnp.where(row == r, read, 0.0).astype(jnp.bfloat16) for r in range(rows)], axis=1
    )


def columns(left, weight_ref, share, out_ref):
    width = out_ref.shape[-1]
    for n in range(0, width, STEP):
        at = pl.ds(pl.multiple_of(share * width + n, STEP), STEP)
        term = jnp.dot(left, weight_ref[:, at], preferred_element_type=jnp.float32)
        out_ref[:, pl.ds(n, STEP)] = jnp.sum(term, axis=0, keepdims=True)


def project_first(away, arrived_ref, weight_ref, left_ref, out_ref):
    left = merge(arrived_ref, weight_ref.shape[0] // HEAD_SIZE)
    left_ref[...] = left
    columns(left, weight_ref, lax.axis_index("group") ^ away, out_ref)


def project_next(away, left_ref, weight_ref, out_ref):
    columns(left_ref[...], weight_ref, lax.axis_index("group") ^ away, out_ref)


def add_all(*refs):
    out_ref = refs[-1]
    total = refs[0][...]
    for ref in refs[1:-1]:
        total = total + ref[...]
    out_ref[...] = total.astype(out_ref.dtype)


def per_device(new_queries, stored_keys, stored_values, used_length, out_weight):
    batch, heads = stored_keys.shape[:2]
    group = new_queries.shape[2]
    rows = heads * group
    width = out_weight.shape[-1]
    vmem = functools.partial(pltpu.with_memory_space_constraint, memory_space=pltpu.VMEM)
    whole = pl.BlockSpec(memory_space=pltpu.VMEM)

    queries = new_queries.reshape(1, rows, HEAD_SIZE)
    copies = pl.pallas_call(
        spread,
        out_shape=jax.ShapeDtypeStruct((batch, rows, HEAD_SIZE), queries.dtype),
        in_specs=[whole],
        out_specs=whole,
        cost_estimate=pl.CostEstimate(flops=10**11, bytes_accessed=10**9, transcendentals=0),
        compiler_params=pltpu.CompilerParams(vmem_limit_bytes=1 << 20),
        name="spread",
    )(queries)
    all_queries = lax.all_to_all(copies, "seq", split_axis=0, concat_axis=0, tiled=True)
    packed = pl.pallas_call(
        attend,
        out_shape=jax.ShapeDtypeStruct((batch * (rows + 1), HEAD_SIZE), jnp.float32),
        in_specs=[whole] * 4,
        out_specs=whole,
        compiler_params=pltpu.CompilerParams(vmem_limit_bytes=8 << 20),
        name="attend",
    )(used_length.reshape(1, batch), vmem(all_queries), vmem(stored_keys), vmem(stored_values))
    arrived = lax.all_to_all(
        packed.reshape(batch, rows + 1, 1, HEAD_SIZE), "seq", split_axis=0, concat_axis=0, tiled=True
    ).reshape(packed.shape)
    shares = lax.axis_size("group")
    piece = jax.ShapeDtypeStruct((1, width // shares), jnp.float32)
    small = pltpu.CompilerParams(vmem_limit_bytes=8 << 20)
    cost = pl.CostEstimate(flops=10**9, bytes_accessed=10**7, transcendentals=0)
    weight = vmem(out_weight.reshape(rows * HEAD_SIZE, width))
    left, term = pl.pallas_call(
        functools.partial(project_first, NEAR ^ LAST),
        out_shape=(jax.ShapeDtypeStruct((rows, rows * HEAD_SIZE), jnp.bfloat16), piece),
        in_specs=[whole, whole],
        out_specs=(whole, whole),
        compiler_params=small,
        name="project_first",
    )(vmem(arrived), weight)

    def send(term, away):
        return lax.ppermute(term, "group", [(j, j ^ away) for j in range(shares)])

    def following(away):
        return pl.pallas_call(
            functools.partial(project_next, away),
            out_shape=piece,
            in_specs=[whole, whole],
            out_specs=whole,
            cost_estimate=cost,
            compiler_params=small,
            name="project_next",
        )(left, weight)

    def added(parts, dtype):
        return pl.pallas_call(
            add_all,
            out_shape=jax.ShapeDtypeStruct(piece.shape, dtype),
            in_specs=[whole] * len(parts),
            out_specs=whole,
            compiler_params=small,
        )(*parts)

    passed = send(term, NEAR)
    direct = send(following(NEAR), NEAR)
    beyond = following(LAST)
    last = send(added([beyond, passed], jnp.float32), LAST)
    own = following(0)
    return added([own, direct, last], jnp.bfloat16)


def solution(mesh):
    in_specs = (
        P("seq", "group", None, None),
        P(None, "group", "seq", None),
        P(None, "group", "seq", None),
        P(),
        P("group", None, None, None),
    )
    out_specs = P("seq", "group")
    return jax.shard_map(
        per_device, mesh=mesh, in_specs=in_specs, out_specs=out_specs, check_vma=False
    )
```

```python
import functools

import jax
import jax.numpy as jnp
from jax import lax
from jax.experimental import pallas as pl
from jax.experimental.pallas import tpu as pltpu
from jax.sharding import PartitionSpec as P

HEAD_SIZE = 128
EMPTY = -4000.0
TINY = 1e-30
SPAN = 16384.0
LOG2_E = 1.4426950408889634
STEP = 256
NEAR, LAST = 1, 3
TO_BASE_2 = HEAD_SIZE ** (-0.5) * LOG2_E


def log2(x):
    return jnp.log(x) * LOG2_E


def split(x):
    first = jnp.floor(x * 0.25 + 0.5)
    x = x - first * 4.0
    second = jnp.floor(x * 2.0**9 + 0.5)
    x = x - second * 2.0**-9
    return first, second, jnp.floor(x * 2.0**20 + 0.5)


def attend(used_ref, query_ref, key_ref, value_ref, out_ref):
    batch, heads, width, _ = key_ref.shape
    rows = query_ref.shape[1]
    group = rows // heads
    first = lax.axis_index("seq") * width
    lane = lax.broadcasted_iota(jnp.int32, (rows, HEAD_SIZE), 1)
    row = lax.broadcasted_iota(jnp.int32, (rows, HEAD_SIZE), 0)
    place = lax.broadcasted_iota(jnp.int32, (rows, width), 1)

    def side_by_side(ref, b):
        return jnp.concatenate([ref[b, k] for k in range(heads)], axis=1)

    used = used_ref[...] - first
    at = range(batch)
    logits = []
    for b in at:
        query = query_ref[b].astype(jnp.float32)
        left = jnp.concatenate(
            [jnp.where(row // group == k, query, 0.0) for k in range(heads)], axis=1
        ).astype(jnp.bfloat16)
        logits.append(
            lax.dot_general(
                left, side_by_side(key_ref, b), (((1,), (1,)), ((), ())),
                preferred_element_type=jnp.float32,
            )
        )
    filled = [place < used[:, b : b + 1] for b in at]
    logits = [jnp.where(f, x * TO_BASE_2, EMPTY) for f, x in zip(filled, logits)]
    tops = [jnp.max(x, axis=1, keepdims=True) for x in logits]
    parts = [jnp.where(f, jnp.exp2(x - t), 0.0) for f, x, t in zip(filled, logits, tops)]
    totals = [jnp.sum(p, axis=1, keepdims=True) for p in parts]
    reads = []
    for b, part in zip(at, parts):
        high = part.astype(jnp.bfloat16)
        low = (part - high.astype(jnp.float32)).astype(jnp.bfloat16)
        both = jnp.dot(
            jnp.concatenate([high, low], axis=0), side_by_side(value_ref, b),
            preferred_element_type=jnp.float32,
        )
        reads.append(both[:rows] + both[rows:])
    for b, read, top, total in zip(at, reads, tops, totals):
        read = jnp.concatenate(
            [
                read[k * group : (k + 1) * group, k * HEAD_SIZE : (k + 1) * HEAD_SIZE]
                for k in range(heads)
            ],
            axis=0,
        )
        largest = jnp.maximum(jnp.max(jnp.abs(read), axis=1, keepdims=True), TINY)
        out_ref[pl.ds(b * (rows + 2), rows), :] = read * (SPAN / largest)
        pieces = split(top + log2(largest / SPAN)) + split(top + log2(jnp.maximum(total, TINY)))
        stats = jnp.zeros((rows, HEAD_SIZE), jnp.float32)
        for i, piece in enumerate(pieces):
            stats = jnp.where(lane == row + i * rows, piece, stats)
        out_ref[pl.ds(b * (rows + 2) + rows, 2), :] = jnp.broadcast_to(
            jnp.sum(stats, axis=0, keepdims=True), (2, HEAD_SIZE)
        )


def spread(one_ref, out_ref):
    out_ref[...] = jnp.broadcast_to(one_ref[...], out_ref.shape)


def merge(arrived_ref, rows):
    sources = arrived_ref.shape[0] // (rows + 2)
    stats = arrived_ref[pl.ds(rows, sources, stride=rows + 2), :]
    stats = (
        stats * 4.0
        + pltpu.roll(stats, HEAD_SIZE - rows, 1) * 2.0**-9
        + pltpu.roll(stats, HEAD_SIZE - 2 * rows, 1) * 2.0**-20
    )
    mine = lax.broadcasted_iota(jnp.int32, stats.shape, 1) < rows
    sums = jnp.where(mine, pltpu.roll(stats, HEAD_SIZE - 3 * rows, 1), 0.0)
    tops = jnp.where(mine, stats, 0.0)
    most = jnp.max(sums, axis=0, keepdims=True)
    scale = jnp.exp2(tops - most) / jnp.sum(jnp.exp2(sums - most), axis=0, keepdims=True)
    scale = jnp.transpose(scale)[:rows]
    terms = [
        arrived_ref[pl.ds(s * (rows + 2), rows), :] * scale[:, s : s + 1] for s in range(sources)
    ]
    while len(terms) > 1:
        terms = [a + b for a, b in zip(terms[::2], terms[1::2])]
    read = terms[0]
    row = lax.broadcasted_iota(jnp.int32, (rows, HEAD_SIZE), 0)
    return jnp.concatenate(
        [jnp.where(row == r, read, 0.0).astype(jnp.bfloat16) for r in range(rows)], axis=1
    )


def columns(left, weight_ref, share, out_ref):
    width = out_ref.shape[-1]
    for n in range(0, width, STEP):
        at = pl.ds(pl.multiple_of(share * width + n, STEP), STEP)
        term = jnp.dot(left, weight_ref[:, at], preferred_element_type=jnp.float32)
        out_ref[:, pl.ds(n, STEP)] = jnp.sum(term, axis=0, keepdims=True)


def project_first(away, arrived_ref, weight_ref, left_ref, out_ref):
    left = merge(arrived_ref, weight_ref.shape[0] // HEAD_SIZE)
    left_ref[...] = left
    columns(left, weight_ref, lax.axis_index("group") ^ away, out_ref)


def project_next(away, left_ref, weight_ref, out_ref):
    columns(left_ref[...], weight_ref, lax.axis_index("group") ^ away, out_ref)


def add_all(*refs):
    out_ref = refs[-1]
    total = refs[0][...]
    for ref in refs[1:-1]:
        total = total + ref[...]
    out_ref[...] = total.astype(out_ref.dtype)


def per_device(new_queries, stored_keys, stored_values, used_length, out_weight):
    batch, heads = stored_keys.shape[:2]
    group = new_queries.shape[2]
    rows = heads * group
    width = out_weight.shape[-1]
    vmem = functools.partial(pltpu.with_memory_space_constraint, memory_space=pltpu.VMEM)
    whole = pl.BlockSpec(memory_space=pltpu.VMEM)

    queries = new_queries.reshape(1, rows, HEAD_SIZE)
    copies = pl.pallas_call(
        spread,
        out_shape=jax.ShapeDtypeStruct((batch, rows, HEAD_SIZE), queries.dtype),
        in_specs=[whole],
        out_specs=whole,
        cost_estimate=pl.CostEstimate(flops=10**11, bytes_accessed=10**9, transcendentals=0),
        compiler_params=pltpu.CompilerParams(vmem_limit_bytes=1 << 20),
        name="spread",
    )(queries)
    all_queries = lax.all_to_all(copies, "seq", split_axis=0, concat_axis=0, tiled=True)
    packed = pl.pallas_call(
        attend,
        out_shape=jax.ShapeDtypeStruct((batch * (rows + 2), HEAD_SIZE), jnp.float32),
        in_specs=[whole] * 4,
        out_specs=whole,
        compiler_params=pltpu.CompilerParams(vmem_limit_bytes=8 << 20),
        name="attend",
    )(used_length.reshape(1, batch), vmem(all_queries), vmem(stored_keys), vmem(stored_values))
    halves = packed.astype(jnp.float16).reshape(batch, (rows + 2) // 2, 2, HEAD_SIZE)
    halves = lax.all_to_all(halves, "seq", split_axis=0, concat_axis=0, tiled=True)
    arrived = halves.reshape(packed.shape).astype(jnp.float32)
    shares = lax.axis_size("group")
    piece = jax.ShapeDtypeStruct((1, width // shares), jnp.float32)
    small = pltpu.CompilerParams(vmem_limit_bytes=8 << 20)
    cost = pl.CostEstimate(flops=10**9, bytes_accessed=10**7, transcendentals=0)
    weight = vmem(out_weight.reshape(rows * HEAD_SIZE, width))
    left, term = pl.pallas_call(
        functools.partial(project_first, NEAR ^ LAST),
        out_shape=(jax.ShapeDtypeStruct((rows, rows * HEAD_SIZE), jnp.bfloat16), piece),
        in_specs=[whole, whole],
        out_specs=(whole, whole),
        compiler_params=small,
        name="project_first",
    )(vmem(arrived), weight)

    def send(term, away):
        return lax.ppermute(term, "group", [(j, j ^ away) for j in range(shares)])

    def following(away):
        return pl.pallas_call(
            functools.partial(project_next, away),
            out_shape=piece,
            in_specs=[whole, whole],
            out_specs=whole,
            cost_estimate=cost,
            compiler_params=small,
            name="project_next",
        )(left, weight)

    def added(parts, dtype):
        return pl.pallas_call(
            add_all,
            out_shape=jax.ShapeDtypeStruct(piece.shape, dtype),
            in_specs=[whole] * len(parts),
            out_specs=whole,
            compiler_params=small,
        )(*parts)

    passed = send(term, NEAR)
    direct = send(following(NEAR), NEAR)
    beyond = following(LAST)
    last = send(added([beyond, passed], jnp.float32), LAST)
    own = following(0)
    return added([own, direct, last], jnp.bfloat16)


def solution(mesh):
    in_specs = (
        P("seq", "group", None, None),
        P(None, "group", "seq", None),
        P(None, "group", "seq", None),
        P(),
        P("group", None, None, None),
    )
    out_specs = P("seq", "group")
    return jax.shard_map(
        per_device, mesh=mesh, in_specs=in_specs, out_specs=out_specs, check_vma=False
    )
```

```python
import functools

import jax
import jax.numpy as jnp
from jax import lax
from jax.experimental import pallas as pl
from jax.experimental.pallas import tpu as pltpu
from jax.sharding import PartitionSpec as P

HEAD_SIZE = 128
EMPTY = -4000.0
TINY = 1e-30
SPAN = 28.99
LOWEST = -13.0
LOG2_E = 1.4426950408889634
STEP = 256
NEAR, LAST = 1, 3
TO_BASE_2 = HEAD_SIZE ** (-0.5) * LOG2_E


def log2(x):
    return jnp.log(x) * LOG2_E


def split(x):
    first = jnp.floor(x * 0.25 + 0.5)
    x = x - first * 4.0
    second = jnp.floor(x * 2.0**9 + 0.5)
    x = x - second * 2.0**-9
    return first, second, jnp.floor(x * 2.0**20 + 0.5)


def encode(x):
    size = jnp.abs(x)
    whole = jnp.floor(size)
    code = jnp.exp2(whole + LOWEST) * (1.0 + (size - whole))
    return jnp.where(x < 0.0, -code, code)


def decode(code):
    size = jnp.abs(code)
    power = jnp.floor(log2(size))
    x = power - LOWEST + (size * jnp.exp2(-power) - 1.0)
    return jnp.where(code < 0.0, -x, x)


def attend(used_ref, query_ref, key_ref, value_ref, out_ref):
    batch, heads, width, _ = key_ref.shape
    rows = query_ref.shape[1]
    group = rows // heads
    first = lax.axis_index("seq") * width
    lane = lax.broadcasted_iota(jnp.int32, (rows, HEAD_SIZE), 1)
    row = lax.broadcasted_iota(jnp.int32, (rows, HEAD_SIZE), 0)
    place = lax.broadcasted_iota(jnp.int32, (rows, width), 1)

    def side_by_side(ref, b):
        return jnp.concatenate([ref[b, k] for k in range(heads)], axis=1)

    used = used_ref[...] - first
    at = range(batch)
    logits = []
    for b in at:
        query = query_ref[b].astype(jnp.float32)
        left = jnp.concatenate(
            [jnp.where(row // group == k, query, 0.0) for k in range(heads)], axis=1
        ).astype(jnp.bfloat16)
        logits.append(
            lax.dot_general(
                left, side_by_side(key_ref, b), (((1,), (1,)), ((), ())),
                preferred_element_type=jnp.float32,
            )
        )
    filled = [place < used[:, b : b + 1] for b in at]
    logits = [jnp.where(f, x * TO_BASE_2, EMPTY) for f, x in zip(filled, logits)]
    tops = [jnp.max(x, axis=1, keepdims=True) for x in logits]
    parts = [jnp.where(f, jnp.exp2(x - t), 0.0) for f, x, t in zip(filled, logits, tops)]
    totals = [jnp.sum(p, axis=1, keepdims=True) for p in parts]
    reads = []
    for b, part in zip(at, parts):
        high = part.astype(jnp.bfloat16)
        low = (part - high.astype(jnp.float32)).astype(jnp.bfloat16)
        both = jnp.dot(
            jnp.concatenate([high, low], axis=0), side_by_side(value_ref, b),
            preferred_element_type=jnp.float32,
        )
        reads.append(both[:rows] + both[rows:])
    for b, read, top, total in zip(at, reads, tops, totals):
        read = jnp.concatenate(
            [
                read[k * group : (k + 1) * group, k * HEAD_SIZE : (k + 1) * HEAD_SIZE]
                for k in range(heads)
            ],
            axis=0,
        )
        largest = jnp.maximum(jnp.max(jnp.abs(read), axis=1, keepdims=True), TINY)
        out_ref[pl.ds(b * (rows + 2), rows), :] = encode(read * (SPAN / largest))
        pieces = split(top + log2(largest / SPAN)) + split(top + log2(jnp.maximum(total, TINY)))
        stats = jnp.zeros((rows, HEAD_SIZE), jnp.float32)
        for i, piece in enumerate(pieces):
            stats = jnp.where(lane == row + i * rows, piece, stats)
        out_ref[pl.ds(b * (rows + 2) + rows, 2), :] = jnp.broadcast_to(
            jnp.sum(stats, axis=0, keepdims=True), (2, HEAD_SIZE)
        )


def spread(one_ref, out_ref):
    out_ref[...] = jnp.broadcast_to(one_ref[...], out_ref.shape)


def merge(arrived_ref, rows):
    sources = arrived_ref.shape[0] // (rows + 2)
    stats = arrived_ref[pl.ds(rows, sources, stride=rows + 2), :]
    stats = (
        stats * 4.0
        + pltpu.roll(stats, HEAD_SIZE - rows, 1) * 2.0**-9
        + pltpu.roll(stats, HEAD_SIZE - 2 * rows, 1) * 2.0**-20
    )
    mine = lax.broadcasted_iota(jnp.int32, stats.shape, 1) < rows
    sums = jnp.where(mine, pltpu.roll(stats, HEAD_SIZE - 3 * rows, 1), 0.0)
    tops = jnp.where(mine, stats, 0.0)
    most = jnp.max(sums, axis=0, keepdims=True)
    scale = jnp.exp2(tops - most) / jnp.sum(jnp.exp2(sums - most), axis=0, keepdims=True)
    scale = jnp.transpose(scale)[:rows]
    terms = [
        decode(arrived_ref[pl.ds(s * (rows + 2), rows), :]) * scale[:, s : s + 1]
        for s in range(sources)
    ]
    while len(terms) > 1:
        terms = [a + b for a, b in zip(terms[::2], terms[1::2])]
    read = terms[0]
    row = lax.broadcasted_iota(jnp.int32, (rows, HEAD_SIZE), 0)
    return jnp.concatenate(
        [jnp.where(row == r, read, 0.0).astype(jnp.bfloat16) for r in range(rows)], axis=1
    )


def columns(left, weight_ref, share, out_ref):
    width = out_ref.shape[-1]
    for n in range(0, width, STEP):
        at = pl.ds(pl.multiple_of(share * width + n, STEP), STEP)
        term = jnp.dot(left, weight_ref[:, at], preferred_element_type=jnp.float32)
        out_ref[:, pl.ds(n, STEP)] = jnp.sum(term, axis=0, keepdims=True)


def project_first(away, arrived_ref, weight_ref, left_ref, out_ref):
    left = merge(arrived_ref, weight_ref.shape[0] // HEAD_SIZE)
    left_ref[...] = left
    columns(left, weight_ref, lax.axis_index("group") ^ away, out_ref)


def project_next(away, left_ref, weight_ref, out_ref):
    columns(left_ref[...], weight_ref, lax.axis_index("group") ^ away, out_ref)


def add_all(*refs):
    out_ref = refs[-1]
    total = refs[0][...]
    for ref in refs[1:-1]:
        total = total + ref[...]
    out_ref[...] = total.astype(out_ref.dtype)


def per_device(new_queries, stored_keys, stored_values, used_length, out_weight):
    batch, heads = stored_keys.shape[:2]
    group = new_queries.shape[2]
    rows = heads * group
    width = out_weight.shape[-1]
    vmem = functools.partial(pltpu.with_memory_space_constraint, memory_space=pltpu.VMEM)
    whole = pl.BlockSpec(memory_space=pltpu.VMEM)

    queries = new_queries.reshape(1, rows, HEAD_SIZE)
    copies = pl.pallas_call(
        spread,
        out_shape=jax.ShapeDtypeStruct((batch, rows, HEAD_SIZE), queries.dtype),
        in_specs=[whole],
        out_specs=whole,
        cost_estimate=pl.CostEstimate(flops=10**11, bytes_accessed=10**9, transcendentals=0),
        compiler_params=pltpu.CompilerParams(vmem_limit_bytes=1 << 20),
        name="spread",
    )(queries)
    all_queries = lax.all_to_all(copies, "seq", split_axis=0, concat_axis=0, tiled=True)
    packed = pl.pallas_call(
        attend,
        out_shape=jax.ShapeDtypeStruct((batch * (rows + 2), HEAD_SIZE), jnp.float32),
        in_specs=[whole] * 4,
        out_specs=whole,
        compiler_params=pltpu.CompilerParams(vmem_limit_bytes=8 << 20),
        name="attend",
    )(used_length.reshape(1, batch), vmem(all_queries), vmem(stored_keys), vmem(stored_values))
    halves = packed.astype(jnp.float16).reshape(batch, (rows + 2) // 2, 2, HEAD_SIZE)
    halves = lax.all_to_all(halves, "seq", split_axis=0, concat_axis=0, tiled=True)
    arrived = halves.reshape(packed.shape).astype(jnp.float32)
    shares = lax.axis_size("group")
    piece = jax.ShapeDtypeStruct((1, width // shares), jnp.float32)
    small = pltpu.CompilerParams(vmem_limit_bytes=8 << 20)
    cost = pl.CostEstimate(flops=10**9, bytes_accessed=10**7, transcendentals=0)
    weight = vmem(out_weight.reshape(rows * HEAD_SIZE, width))
    left, term = pl.pallas_call(
        functools.partial(project_first, NEAR ^ LAST),
        out_shape=(jax.ShapeDtypeStruct((rows, rows * HEAD_SIZE), jnp.bfloat16), piece),
        in_specs=[whole, whole],
        out_specs=(whole, whole),
        compiler_params=small,
        name="project_first",
    )(vmem(arrived), weight)

    def send(term, away):
        return lax.ppermute(term, "group", [(j, j ^ away) for j in range(shares)])

    def following(away):
        return pl.pallas_call(
            functools.partial(project_next, away),
            out_shape=piece,
            in_specs=[whole, whole],
            out_specs=whole,
            cost_estimate=cost,
            compiler_params=small,
            name="project_next",
        )(left, weight)

    def added(parts, dtype):
        return pl.pallas_call(
            add_all,
            out_shape=jax.ShapeDtypeStruct(piece.shape, dtype),
            in_specs=[whole] * len(parts),
            out_specs=whole,
            compiler_params=small,
        )(*parts)

    passed = send(term, NEAR)
    direct = send(following(NEAR), NEAR)
    beyond = following(LAST)
    last = send(added([beyond, passed], jnp.float32), LAST)
    own = following(0)
    return added([own, direct, last], jnp.bfloat16)


def solution(mesh):
    in_specs = (
        P("seq", "group", None, None),
        P(None, "group", "seq", None),
        P(None, "group", "seq", None),
        P(),
        P("group", None, None, None),
    )
    out_specs = P("seq", "group")
    return jax.shard_map(
        per_device, mesh=mesh, in_specs=in_specs, out_specs=out_specs, check_vma=False
    )
```

```python
import functools

import jax
import jax.numpy as jnp
from jax import lax
from jax.experimental import pallas as pl
from jax.experimental.pallas import tpu as pltpu
from jax.sharding import PartitionSpec as P

HEAD_SIZE = 128
EMPTY = -4000.0
TINY = 1e-30
SPAN = 28.99
LOWEST = -13.0
LOG2_E = 1.4426950408889634
STEP = 256
NEAR, LAST = 1, 3
TO_BASE_2 = HEAD_SIZE ** (-0.5) * LOG2_E


def log2(x):
    return jnp.log(x) * LOG2_E


def split(x):
    first = jnp.floor(x * 0.25 + 0.5)
    x = x - first * 4.0
    second = jnp.floor(x * 2.0**9 + 0.5)
    x = x - second * 2.0**-9
    return first, second, jnp.floor(x * 2.0**20 + 0.5)


def encode(x):
    size = jnp.abs(x)
    whole = jnp.floor(size)
    code = jnp.exp2(whole + LOWEST) * (1.0 + (size - whole))
    return jnp.where(x < 0.0, -code, code)


def decode(code):
    size = jnp.abs(code)
    power = jnp.floor(log2(size))
    x = power - LOWEST + (size * jnp.exp2(-power) - 1.0)
    return jnp.where(code < 0.0, -x, x)


def attend(used_ref, query_ref, key_ref, value_ref, out_ref):
    batch, heads, width, _ = key_ref.shape
    rows = query_ref.shape[1]
    group = rows // heads
    first = lax.axis_index("seq") * width
    lane = lax.broadcasted_iota(jnp.int32, (rows, HEAD_SIZE), 1)
    row = lax.broadcasted_iota(jnp.int32, (rows, HEAD_SIZE), 0)
    place = lax.broadcasted_iota(jnp.int32, (rows, width), 1)

    def side_by_side(ref, b):
        return jnp.concatenate([ref[b, k] for k in range(heads)], axis=1)

    used = used_ref[...] - first
    at = range(batch)
    logits = []
    for b in at:
        query = query_ref[b].astype(jnp.float32)
        left = jnp.concatenate(
            [jnp.where(row // group == k, query, 0.0) for k in range(heads)], axis=1
        ).astype(jnp.bfloat16)
        logits.append(
            lax.dot_general(
                left, side_by_side(key_ref, b), (((1,), (1,)), ((), ())),
                preferred_element_type=jnp.float32,
            )
        )
    filled = [place < used[:, b : b + 1] for b in at]
    logits = [jnp.where(f, x * TO_BASE_2, EMPTY) for f, x in zip(filled, logits)]
    tops = [jnp.maximum(jnp.max(x, axis=1, keepdims=True), 0.5 * EMPTY) for x in logits]
    parts = [jnp.exp2(x - t) for x, t in zip(logits, tops)]
    totals = [jnp.sum(p, axis=1, keepdims=True) for p in parts]
    for b, part, top, total in zip(at, parts, tops, totals):
        high = part.astype(jnp.bfloat16)
        low = (part - high.astype(jnp.float32)).astype(jnp.bfloat16)
        both = jnp.dot(
            jnp.concatenate([high, low], axis=0), side_by_side(value_ref, b),
            preferred_element_type=jnp.float32,
        )
        read = both[:rows] + both[rows:]
        read = jnp.concatenate(
            [
                read[k * group : (k + 1) * group, k * HEAD_SIZE : (k + 1) * HEAD_SIZE]
                for k in range(heads)
            ],
            axis=0,
        )
        largest = jnp.maximum(jnp.max(jnp.abs(read), axis=1, keepdims=True), TINY)
        out_ref[pl.ds(b * (rows + 2), rows), :] = encode(read * (SPAN / largest))
        pieces = split(top + log2(largest / SPAN)) + split(top + log2(jnp.maximum(total, TINY)))
        stats = jnp.zeros((rows, HEAD_SIZE), jnp.float32)
        for i, piece in enumerate(pieces):
            stats = jnp.where(lane == row + i * rows, piece, stats)
        out_ref[pl.ds(b * (rows + 2) + rows, 2), :] = jnp.broadcast_to(
            jnp.sum(stats, axis=0, keepdims=True), (2, HEAD_SIZE)
        )


def spread(one_ref, out_ref):
    out_ref[...] = jnp.broadcast_to(one_ref[...], out_ref.shape)


def merge(arrived_ref, rows):
    sources = arrived_ref.shape[0] // (rows + 2)
    stats = arrived_ref[pl.ds(rows, sources, stride=rows + 2), :]
    stats = (
        stats * 4.0
        + pltpu.roll(stats, HEAD_SIZE - rows, 1) * 2.0**-9
        + pltpu.roll(stats, HEAD_SIZE - 2 * rows, 1) * 2.0**-20
    )
    mine = lax.broadcasted_iota(jnp.int32, stats.shape, 1) < rows
    sums = jnp.where(mine, pltpu.roll(stats, HEAD_SIZE - 3 * rows, 1), 0.0)
    tops = jnp.where(mine, stats, 0.0)
    most = jnp.max(sums, axis=0, keepdims=True)
    scale = jnp.exp2(tops - most) / jnp.sum(jnp.exp2(sums - most), axis=0, keepdims=True)
    scale = jnp.transpose(scale)[:rows]
    terms = [
        decode(arrived_ref[pl.ds(s * (rows + 2), rows), :]) * scale[:, s : s + 1]
        for s in range(sources)
    ]
    while len(terms) > 1:
        terms = [a + b for a, b in zip(terms[::2], terms[1::2])]
    read = terms[0]
    row = lax.broadcasted_iota(jnp.int32, (rows, HEAD_SIZE), 0)
    return jnp.concatenate(
        [jnp.where(row == r, read, 0.0).astype(jnp.bfloat16) for r in range(rows)], axis=1
    )


def columns(left, weight_ref, share, out_ref):
    width = out_ref.shape[-1]
    for n in range(0, width, STEP):
        at = pl.ds(pl.multiple_of(share * width + n, STEP), STEP)
        term = jnp.dot(left, weight_ref[:, at], preferred_element_type=jnp.float32)
        out_ref[:, pl.ds(n, STEP)] = jnp.sum(term, axis=0, keepdims=True)


def project_first(away, arrived_ref, weight_ref, left_ref, out_ref):
    left = merge(arrived_ref, weight_ref.shape[0] // HEAD_SIZE)
    left_ref[...] = left
    columns(left, weight_ref, lax.axis_index("group") ^ away, out_ref)


def project_next(away, left_ref, weight_ref, out_ref):
    columns(left_ref[...], weight_ref, lax.axis_index("group") ^ away, out_ref)


def add_all(*refs):
    out_ref = refs[-1]
    total = refs[0][...]
    for ref in refs[1:-1]:
        total = total + ref[...]
    out_ref[...] = total.astype(out_ref.dtype)


def per_device(new_queries, stored_keys, stored_values, used_length, out_weight):
    batch, heads = stored_keys.shape[:2]
    group = new_queries.shape[2]
    rows = heads * group
    width = out_weight.shape[-1]
    vmem = functools.partial(pltpu.with_memory_space_constraint, memory_space=pltpu.VMEM)
    whole = pl.BlockSpec(memory_space=pltpu.VMEM)

    queries = new_queries.reshape(1, rows, HEAD_SIZE)
    copies = pl.pallas_call(
        spread,
        out_shape=jax.ShapeDtypeStruct((batch, rows, HEAD_SIZE), queries.dtype),
        in_specs=[whole],
        out_specs=whole,
        cost_estimate=pl.CostEstimate(flops=10**11, bytes_accessed=10**9, transcendentals=0),
        compiler_params=pltpu.CompilerParams(vmem_limit_bytes=1 << 20),
        name="spread",
    )(queries)
    all_queries = lax.all_to_all(copies, "seq", split_axis=0, concat_axis=0, tiled=True)
    packed = pl.pallas_call(
        attend,
        out_shape=jax.ShapeDtypeStruct((batch * (rows + 2), HEAD_SIZE), jnp.float32),
        in_specs=[whole] * 4,
        out_specs=whole,
        compiler_params=pltpu.CompilerParams(vmem_limit_bytes=8 << 20),
        name="attend",
    )(used_length.reshape(1, batch), vmem(all_queries), vmem(stored_keys), vmem(stored_values))
    halves = packed.astype(jnp.float16).reshape(batch, (rows + 2) // 2, 2, HEAD_SIZE)
    halves = lax.all_to_all(halves, "seq", split_axis=0, concat_axis=0, tiled=True)
    arrived = halves.reshape(packed.shape).astype(jnp.float32)
    shares = lax.axis_size("group")
    piece = jax.ShapeDtypeStruct((1, width // shares), jnp.float32)
    small = pltpu.CompilerParams(vmem_limit_bytes=8 << 20)
    cost = pl.CostEstimate(flops=10**9, bytes_accessed=10**7, transcendentals=0)
    weight = vmem(out_weight.reshape(rows * HEAD_SIZE, width))
    left, term = pl.pallas_call(
        functools.partial(project_first, NEAR ^ LAST),
        out_shape=(jax.ShapeDtypeStruct((rows, rows * HEAD_SIZE), jnp.bfloat16), piece),
        in_specs=[whole, whole],
        out_specs=(whole, whole),
        compiler_params=small,
        name="project_first",
    )(vmem(arrived), weight)

    def send(term, away):
        return lax.ppermute(term, "group", [(j, j ^ away) for j in range(shares)])

    def following(away):
        return pl.pallas_call(
            functools.partial(project_next, away),
            out_shape=piece,
            in_specs=[whole, whole],
            out_specs=whole,
            cost_estimate=cost,
            compiler_params=small,
            name="project_next",
        )(left, weight)

    def added(parts, dtype):
        return pl.pallas_call(
            add_all,
            out_shape=jax.ShapeDtypeStruct(piece.shape, dtype),
            in_specs=[whole] * len(parts),
            out_specs=whole,
            compiler_params=small,
        )(*parts)

    passed = send(term, NEAR)
    direct = send(following(NEAR), NEAR)
    beyond = following(LAST)
    last = send(added([beyond, passed], jnp.float32), LAST)
    own = following(0)
    return added([own, direct, last], jnp.bfloat16)


def solution(mesh):
    in_specs = (
        P("seq", "group", None, None),
        P(None, "group", "seq", None),
        P(None, "group", "seq", None),
        P(),
        P("group", None, None, None),
    )
    out_specs = P("seq", "group")
    return jax.shard_map(
        per_device, mesh=mesh, in_specs=in_specs, out_specs=out_specs, check_vma=False
    )
```
